32 devices in a mesh: grp: 2 (over x), lat: 16 (over z, y, core).
Axes of the slice: x: 2, y: 2, z: 4, core: 2. Of those that a mesh axis runs over, the one named last changes fastest.
Arguments:
- acts: bfloat16 [128, 2, 2048], P(('grp', 'lat')), parts along dimension 0, may hold values from -6 to 6
- enc_weight: bfloat16 [4, 2048, 4096], P('grp', None, 'lat'), parts along dimension 0, may hold values from -0.09375 to 0.09375
- enc_bias: float32 [8192], P(('grp', 'lat')), parts along dimension 0, may hold values from -3 to 3
- dec_weight: bfloat16 [4096, 4, 2048], P('lat', 'grp'), parts along dimension 1, may hold values from -0.125 to 0.125
- dec_bias: float32 [4, 2048], P('grp'), parts along dimension 0, may hold values from -5 to 5
Outputs:
- residual: bfloat16 [128, 2, 2048], P(('grp', 'lat')), parts along dimension 0
- grad_enc: bfloat16 [4, 2048, 4096], P('grp', None, 'lat'), parts along dimension 0
- grad_enc_bias: float32 [8192], P(('grp', 'lat')), parts along dimension 0
- grad_dec: bfloat16 [4096, 4, 2048], P('lat', 'grp'), parts along dimension 1
- grad_dec_bias: float32 [4, 2048], P('grp'), parts along dimension 0
The draws below stay inside these ranges and needn't reach their ends.
There are 2 independent parts, one for each index of `grp`. The reference program is written for one: setup_inputs(seed, part) draws one part's arguments, and reference() takes and returns one part's arrays. A program takes and returns all parts, laid end to end along the dimension named above; each array names one. Nothing has to cross between parts.
All inputs are finite; a program needn't handle non-finite values.
Results may differ from the reference program's by a relative error of at most 0.015.
Values may be sent and summed in bfloat16 or wider, within the bound.
No kernel may reach another device: no remote copies, remote signals or barrier semaphores. Data moves between devices by JAX's collectives and lax.ppermute only.
A program may use at most 128 MiB of HBM per device.

```python
import jax
import jax.numpy as jnp
from jax import lax

L = 2
D = 2048
FEATS = 4096
TOKENS = 64


def block_levels(own_key, shape, pieces, low, largest):
    loudness = 1.0
    for dim, blocks in pieces:
        draws = jax.random.uniform(jax.random.fold_in(jax.random.fold_in(own_key, 6), dim), (blocks,), jnp.float32, low / len(pieces), largest / len(pieces))
        loudness = loudness * jnp.repeat(jnp.exp(draws), shape[dim] // blocks).reshape((-1,) + (1,) * (len(shape) - 1 - dim))
    return loudness


def noise(key, extent, deviation, limit, split=(), kind=jnp.bfloat16):
    factor_of = block_levels(key, extent, split, -0.22, 0.18) if split else 1.0
    values = jax.random.normal(key, extent, jnp.float32) * deviation * factor_of
    return jnp.minimum(jnp.maximum(values, -limit), limit).astype(kind)


def setup_inputs(seed: int = 0, part: int = 0) -> dict:
    streams_of = jax.random.split(jax.random.key(seed), 6)
    part_splits = jax.random.split(jax.random.fold_in(streams_of[5], part), 6)
    return {
        "acts": noise(part_splits[0], (TOKENS, L, D), 1.0, 6.0, ((0, 16),)),
        "enc_weight": noise(part_splits[1], (L, D, FEATS), (L * D) ** -0.5, 0.09375, ((2, 16),)),
        "enc_bias": noise(part_splits[2], (FEATS,), 0.5, 3.0, ((0, 16),), jnp.float32),
        "dec_weight": noise(part_splits[3], (FEATS, L, D), D ** -0.5, 0.125, ((0, 16),)),
        "dec_bias": noise(part_splits[4], (L, D), 1.0, 5.0, (), jnp.float32),
    }


sparsity_weight = 2.0

def reference(acts, enc_weight, enc_bias, dec_weight, dec_bias):
    flat_rows = acts.reshape(TOKENS, L * D)
    flat_enc = enc_weight.reshape(L * D, FEATS)
    flat_dec = dec_weight.reshape(FEATS, L * D)
    before = jnp.dot(flat_rows, flat_enc, preferred_element_type=jnp.float32) + enc_bias
    active = jnp.maximum(before, 0.0).astype(jnp.bfloat16)
    rebuilt = jnp.dot(active, flat_dec, preferred_element_type=jnp.float32) + dec_bias.reshape(L * D)
    residual = (rebuilt - flat_rows.astype(jnp.float32)).astype(jnp.bfloat16)
    factor = 2.0 / TOKENS
    dec_wide = dec_weight.astype(jnp.float32)
    row_sq = lax.optimization_barrier(jnp.sum(dec_wide * dec_wide, axis=2))
    inv_norm = lax.rsqrt(row_sq + 1.0)
    dec_norm = lax.optimization_barrier(jnp.sum(jnp.sqrt(row_sq + 1.0), axis=1))
    backward = jnp.dot(residual, flat_dec.T, preferred_element_type=jnp.float32)
    grad_act = factor * backward + sparsity_weight / TOKENS * dec_norm
    grad_before = jnp.where(before > 0.0, grad_act, 0.0).astype(jnp.bfloat16)
    grad_enc = jnp.dot(flat_rows.T, grad_before, preferred_element_type=jnp.float32).astype(jnp.bfloat16).reshape(L, D, FEATS)
    grad_enc_bias = lax.optimization_barrier(jnp.sum(grad_before.astype(jnp.float32), axis=0))
    act_sum = lax.optimization_barrier(jnp.sum(active.astype(jnp.float32), axis=0))
    products = jnp.dot(active.T, residual, preferred_element_type=jnp.float32).reshape(FEATS, L, D)
    grad_dec = (factor * products + sparsity_weight / TOKENS * act_sum[:, None, None] * dec_wide * inv_norm[:, :, None]).astype(jnp.bfloat16)
    grad_dec_bias = (factor * lax.optimization_barrier(jnp.sum(residual.astype(jnp.float32), axis=0))).reshape(L, D)
    return (residual.reshape(TOKENS, L, D), grad_enc, grad_enc_bias, grad_dec, grad_dec_bias)
```

```python
import jax
import jax.numpy as jnp
from jax import lax
from jax.sharding import PartitionSpec as P

sparsity_weight = 2.0


def masks_of(count):
    masks = []
    k = count // 2
    while k:
        masks.append(k)
        k //= 2
    return masks


def swap(x, k, count):
    return lax.ppermute(x, "lat", [(s, s ^ k) for s in range(count)])


def gather_rows(x, count):
    for k in masks_of(count):
        x = jnp.concatenate([x, swap(x, k, count)], axis=0)
    return x


def scatter_rows(term, count):
    for k in reversed(masks_of(count)):
        half = term.shape[0] // 2
        received = swap(term[half:].astype(jnp.bfloat16), k, count)
        term = term[:half] + received.astype(jnp.float32)
    return term


def body(acts, enc_weight, enc_bias, dec_weight, dec_bias):
    tok_dev, layers, width = acts.shape
    lat_dev = enc_weight.shape[2]
    wide = layers * width
    count = lax.axis_size("lat")
    total_rows = tok_dev * count
    factor = 2.0 / total_rows
    flat_rows = acts.reshape(tok_dev, wide)
    flat_enc = enc_weight.reshape(wide, lat_dev)
    flat_dec = lax.optimization_barrier(dec_weight.reshape(lat_dev, wide))
    flat_bias = dec_bias.reshape(wide)
    gathered = gather_rows(flat_rows, count)
    before = jnp.dot(gathered, flat_enc, preferred_element_type=jnp.float32) + enc_bias
    active = jnp.maximum(before, 0.0).astype(jnp.bfloat16)
    term = jnp.dot(active, flat_dec, preferred_element_type=jnp.float32)
    summed = scatter_rows(term, count)
    own_residual = (summed + flat_bias - flat_rows.astype(jnp.float32)).astype(jnp.bfloat16)
    all_residual = gather_rows(own_residual, count)

    layer_dec = [flat_dec[:, l * width : (l + 1) * width].astype(jnp.float32) for l in range(layers)]
    row_sq = [jnp.sum(d * d, axis=1) for d in layer_dec]
    inv_norm = [lax.rsqrt(r + 1.0) for r in row_sq]
    dec_norm = sum(jnp.sqrt(r + 1.0) for r in row_sq)
    gathered_t = lax.optimization_barrier(gathered.T)
    active_t = lax.optimization_barrier(active.T)
    act_sum = jnp.sum(active.astype(jnp.float32), axis=0)

    grad_dec_bias = factor * jnp.sum(all_residual.astype(jnp.float32), axis=0)
    backward = lax.dot_general(
        all_residual, flat_dec, (((1,), (1,)), ((), ())), preferred_element_type=jnp.float32
    )
    grad_act = factor * backward + sparsity_weight / total_rows * dec_norm
    grad_before = jnp.where(before > 0.0, grad_act, 0.0).astype(jnp.bfloat16)
    grad_enc = jnp.dot(gathered_t, grad_before, preferred_element_type=jnp.float32).astype(jnp.bfloat16)
    grad_enc_bias = jnp.sum(grad_before.astype(jnp.float32), axis=0)
    pieces = []
    for l in range(layers):
        total = jnp.dot(
            active_t, all_residual[:, l * width : (l + 1) * width], preferred_element_type=jnp.float32
        )
        scale = sparsity_weight / total_rows * act_sum * inv_norm[l]
        pieces.append((factor * total + scale[:, None] * layer_dec[l]).astype(jnp.bfloat16))
    pieces = lax.optimization_barrier(pieces)
    grad_dec = jnp.stack(pieces, axis=1)
    return (
        own_residual.reshape(tok_dev, layers, width),
        grad_enc.reshape(layers, width, lat_dev),
        grad_enc_bias,
        grad_dec,
        grad_dec_bias.reshape(layers, width),
    )


def solution(mesh):
    return jax.shard_map(
        body,
        mesh=mesh,
        in_specs=(
            P(("grp", "lat"), None, None),
            P("grp", None, "lat"),
            P(("grp", "lat")),
            P("lat", "grp", None),
            P("grp", None),
        ),
        out_specs=(
            P(("grp", "lat"), None, None),
            P("grp", None, "lat"),
            P(("grp", "lat")),
            P("lat", "grp", None),
            P("grp", None),
        ),
        check_vma=False,
    )
```

```python
import jax
import jax.numpy as jnp
from jax import lax
from jax.sharding import PartitionSpec as P

sparsity_weight = 2.0


def masks_of(count):
    masks = []
    k = count // 2
    while k:
        masks.append(k)
        k //= 2
    return masks


def swap(x, k, count):
    return lax.ppermute(x, "lat", [(s, s ^ k) for s in range(count)])


def gather_rows(x, count, direct, side=None):
    masks = masks_of(count)
    if direct and len(masks) > 2:
        far, near = masks[:2]
        parts = [x] + [swap(x, k, count) for k in (far, near, far ^ near)]
        x = jnp.concatenate(parts, axis=0)
        masks = masks[2:]
    for k in masks:
        if side is not None and k == 1:
            x, side = lax.optimization_barrier((x, side))
        x = jnp.concatenate([x, swap(x, k, count)], axis=0)
    return x if side is None else (x, side)


def scatter_rows(term, count, direct):
    masks = masks_of(count)
    last = masks[:2] if direct and len(masks) > 2 else []
    for k in reversed(masks[len(last) :]):
        half = term.shape[0] // 2
        received = swap(term[half:].astype(jnp.bfloat16), k, count)
        term = term[:half] + received.astype(jnp.float32)
    if last:
        far, near = last
        rows = term.shape[0] // 4
        blocks = [term[p * rows : (p + 1) * rows] for p in range(4)]
        got = [swap(b.astype(jnp.bfloat16), k, count) for b, k in zip(blocks[1:], (far, near, far ^ near))]
        term = blocks[0] + sum(g.astype(jnp.float32) for g in got)
    return term


def body(acts, enc_weight, enc_bias, dec_weight, dec_bias):
    tok_dev, layers, width = acts.shape
    lat_dev = enc_weight.shape[2]
    wide = layers * width
    count = lax.axis_size("lat")
    total_rows = tok_dev * count
    factor = 2.0 / total_rows
    flat_rows = acts.reshape(tok_dev, wide)
    flat_enc = enc_weight.reshape(wide, lat_dev)
    flat_dec = lax.optimization_barrier(dec_weight.reshape(lat_dev, wide))
    flat_bias = dec_bias.reshape(wide)
    gathered, flat_dec = gather_rows(flat_rows, count, True, flat_dec)
    before = jnp.dot(gathered, flat_enc, preferred_element_type=jnp.float32) + enc_bias
    active = jnp.maximum(before, 0.0).astype(jnp.bfloat16)
    term = jnp.dot(active, flat_dec, preferred_element_type=jnp.float32)
    summed = scatter_rows(term, count, True)
    own_residual = (summed + flat_bias - flat_rows.astype(jnp.float32)).astype(jnp.bfloat16)
    all_residual = gather_rows(own_residual, count, True)

    layer_dec = [flat_dec[:, l * width : (l + 1) * width].astype(jnp.float32) for l in range(layers)]
    row_sq = [jnp.sum(d * d, axis=1) for d in layer_dec]
    inv_norm = [lax.rsqrt(r + 1.0) for r in row_sq]
    dec_norm = sum(jnp.sqrt(r + 1.0) for r in row_sq)
    gathered_t = lax.optimization_barrier(gathered.T)
    active_t = lax.optimization_barrier(active.T)
    act_sum = jnp.sum(active.astype(jnp.float32), axis=0)

    grad_dec_bias = factor * jnp.sum(all_residual.astype(jnp.float32), axis=0)
    backward = lax.dot_general(
        all_residual, flat_dec, (((1,), (1,)), ((), ())), preferred_element_type=jnp.float32
    )
    grad_act = factor * backward + sparsity_weight / total_rows * dec_norm
    grad_before = jnp.where(before > 0.0, grad_act, 0.0).astype(jnp.bfloat16)
    grad_enc = jnp.dot(gathered_t, grad_before, preferred_element_type=jnp.float32).astype(jnp.bfloat16)
    grad_enc_bias = jnp.sum(grad_before.astype(jnp.float32), axis=0)
    pieces = []
    for l in range(layers):
        total = jnp.dot(
            active_t, all_residual[:, l * width : (l + 1) * width], preferred_element_type=jnp.float32
        )
        scale = sparsity_weight / total_rows * act_sum * inv_norm[l]
        pieces.append((factor * total + scale[:, None] * layer_dec[l]).astype(jnp.bfloat16))
    pieces = lax.optimization_barrier(pieces)
    grad_dec = jnp.stack(pieces, axis=1)
    return (
        own_residual.reshape(tok_dev, layers, width),
        grad_enc.reshape(layers, width, lat_dev),
        grad_enc_bias,
        grad_dec,
        grad_dec_bias.reshape(layers, width),
    )


def solution(mesh):
    return jax.shard_map(
        body,
        mesh=mesh,
        in_specs=(
            P(("grp", "lat"), None, None),
            P("grp", None, "lat"),
            P(("grp", "lat")),
            P("lat", "grp", None),
            P("grp", None),
        ),
        out_specs=(
            P(("grp", "lat"), None, None),
            P("grp", None, "lat"),
            P(("grp", "lat")),
            P("lat", "grp", None),
            P("grp", None),
        ),
        check_vma=False,
    )
```

```python
import jax
import jax.numpy as jnp
from jax import lax
from jax.sharding import PartitionSpec as P

sparsity_weight = 2.0


def masks_of(count):
    masks = []
    k = count // 2
    while k:
        masks.append(k)
        k //= 2
    return masks


def swap(x, k, count):
    return lax.ppermute(x, "lat", [(s, s ^ k) for s in range(count)])


def steps_of(count):
    masks = masks_of(count)
    if len(masks) < 4:
        return [[k] for k in masks]
    return [[k] for k in masks[2:-1]] + [masks[:2], masks[-1:]]


def gather_rows(x, count, direct, side=None):
    for step in steps_of(count):
        if side is not None and step == [1]:
            x, side = lax.optimization_barrier((x, side))
        if len(step) == 2:
            far, near = step
            others = [swap(x, k, count) for k in (far, near, far ^ near)]
        else:
            others = [swap(x, step[0], count)]
        x = jnp.concatenate([x] + others, axis=0)
    return x if side is None else (x, side)


def scatter_rows(term, count, direct):
    for step in reversed(steps_of(count)):
        if len(step) == 2:
            far, near = step
            send = (far, near, far ^ near)
        else:
            send = (step[0],)
        rows = term.shape[0] // (len(send) + 1)
        got = [
            swap(term[p * rows : (p + 1) * rows].astype(jnp.bfloat16), k, count) for p, k in enumerate(send, 1)
        ]
        term = term[:rows] + sum(g.astype(jnp.float32) for g in got)
    return term


def body(acts, enc_weight, enc_bias, dec_weight, dec_bias):
    tok_dev, layers, width = acts.shape
    lat_dev = enc_weight.shape[2]
    wide = layers * width
    count = lax.axis_size("lat")
    total_rows = tok_dev * count
    factor = 2.0 / total_rows
    flat_rows = acts.reshape(tok_dev, wide)
    flat_enc = enc_weight.reshape(wide, lat_dev)
    flat_dec = lax.optimization_barrier(dec_weight.reshape(lat_dev, wide))
    flat_bias = dec_bias.reshape(wide)
    gathered, flat_dec = gather_rows(flat_rows, count, True, flat_dec)
    before = jnp.dot(gathered, flat_enc, preferred_element_type=jnp.float32) + enc_bias
    active = jnp.maximum(before, 0.0).astype(jnp.bfloat16)
    term = jnp.dot(active, flat_dec, preferred_element_type=jnp.float32)
    summed = scatter_rows(term, count, True)
    own_residual = (summed + flat_bias - flat_rows.astype(jnp.float32)).astype(jnp.bfloat16)
    own_residual, dec_t = lax.optimization_barrier((own_residual, flat_dec))
    all_residual, dec_t = gather_rows(own_residual, count, True, lax.optimization_barrier(dec_t.T))

    layer_dec = [flat_dec[:, l * width : (l + 1) * width].astype(jnp.float32) for l in range(layers)]
    row_sq = [jnp.sum(d * d, axis=1) for d in layer_dec]
    inv_norm = [lax.rsqrt(r + 1.0) for r in row_sq]
    dec_norm = sum(jnp.sqrt(r + 1.0) for r in row_sq)
    gathered_t = lax.optimization_barrier(gathered.T)
    active_t = lax.optimization_barrier(active.T)
    act_sum = jnp.sum(active.astype(jnp.float32), axis=0)

    grad_dec_bias = jnp.concatenate(
        [
            factor * jnp.sum(all_residual[:, l * width : (l + 1) * width].astype(jnp.float32), axis=0, keepdims=True)
            for l in range(layers)
        ],
        axis=0,
    )
    backward = jnp.dot(all_residual, dec_t, preferred_element_type=jnp.float32)
    grad_act = factor * backward + sparsity_weight / total_rows * dec_norm
    grad_before = jnp.where(before > 0.0, grad_act, 0.0).astype(jnp.bfloat16)
    grad_enc = jnp.dot(gathered_t, grad_before, preferred_element_type=jnp.float32).astype(jnp.bfloat16)
    grad_enc_bias = jnp.sum(grad_before.astype(jnp.float32), axis=0)
    pieces = []
    for l in range(layers):
        total = jnp.dot(
            active_t, all_residual[:, l * width : (l + 1) * width], preferred_element_type=jnp.float32
        )
        scale = sparsity_weight / total_rows * act_sum * inv_norm[l]
        pieces.append((factor * total + scale[:, None] * layer_dec[l]).astype(jnp.bfloat16))
    pieces = lax.optimization_barrier(pieces)
    grad_dec = jnp.stack(pieces, axis=1)
    return (
        own_residual.reshape(tok_dev, layers, width),
        grad_enc.reshape(layers, width, lat_dev),
        grad_enc_bias,
        grad_dec,
        grad_dec_bias,
    )


def solution(mesh):
    return jax.shard_map(
        body,
        mesh=mesh,
        in_specs=(
            P(("grp", "lat"), None, None),
            P("grp", None, "lat"),
            P(("grp", "lat")),
            P("lat", "grp", None),
            P("grp", None),
        ),
        out_specs=(
            P(("grp", "lat"), None, None),
            P("grp", None, "lat"),
            P(("grp", "lat")),
            P("lat", "grp", None),
            P("grp", None),
        ),
        check_vma=False,
    )
```

```python
import jax
import jax.numpy as jnp
from jax import lax
from jax.sharding import PartitionSpec as P

sparsity_weight = 2.0


def masks_of(count):
    masks = []
    k = count // 2
    while k:
        masks.append(k)
        k //= 2
    return masks


def swap(x, k, count):
    return lax.ppermute(x, "lat", [(s, s ^ k) for s in range(count)])


def steps_of(count):
    masks = masks_of(count)
    if len(masks) < 4:
        return [[k] for k in masks]
    return [[k] for k in masks[2:-1]] + [masks[:2], masks[-1:]]


def gather_rows(x, count, direct, side=None, side_at=2):
    for step in steps_of(count):
        if side is not None and len(step) == side_at:
            x, side = lax.optimization_barrier((x, side))
        if len(step) == 2:
            far, near = step
            others = [swap(x, k, count) for k in (far, near, far ^ near)]
        else:
            others = [swap(x, step[0], count)]
        x = jnp.concatenate([x] + others, axis=0)
    return x if side is None else (x, side)


def scatter_rows(term, count, direct):
    for step in reversed(steps_of(count)):
        if len(step) == 2:
            far, near = step
            send = (far, near, far ^ near)
        else:
            send = (step[0],)
        rows = term.shape[0] // (len(send) + 1)
        got = [
            swap(term[p * rows : (p + 1) * rows].astype(jnp.bfloat16), k, count) for p, k in enumerate(send, 1)
        ]
        term = term[:rows] + sum(g.astype(jnp.float32) for g in got)
    return term


def body(acts, enc_weight, enc_bias, dec_weight, dec_bias):
    tok_dev, layers, width = acts.shape
    lat_dev = enc_weight.shape[2]
    wide = layers * width
    count = lax.axis_size("lat")
    total_rows = tok_dev * count
    factor = 2.0 / total_rows
    flat_rows = acts.reshape(tok_dev, wide)
    flat_enc = enc_weight.reshape(wide, lat_dev)
    flat_dec = lax.optimization_barrier(dec_weight.reshape(lat_dev, wide))
    flat_bias = dec_bias.reshape(wide)
    gathered, flat_dec = gather_rows(flat_rows, count, True, flat_dec)
    before = jnp.dot(gathered, flat_enc, preferred_element_type=jnp.float32) + enc_bias
    active = jnp.maximum(before, 0.0).astype(jnp.bfloat16)
    term = jnp.dot(active, flat_dec, preferred_element_type=jnp.float32)
    summed = scatter_rows(term, count, True)
    own_residual = (summed + flat_bias - flat_rows.astype(jnp.float32)).astype(jnp.bfloat16)
    own_residual, dec_t = lax.optimization_barrier((own_residual, flat_dec))
    all_residual, dec_t = gather_rows(own_residual, count, True, lax.optimization_barrier(dec_t.T), 1)

    layer_dec = [flat_dec[:, l * width : (l + 1) * width].astype(jnp.float32) for l in range(layers)]
    row_sq = [jnp.sum(d * d, axis=1) for d in layer_dec]
    inv_norm = [lax.rsqrt(r + 1.0) for r in row_sq]
    dec_norm = sum(jnp.sqrt(r + 1.0) for r in row_sq)
    gathered_t = lax.optimization_barrier(gathered.T)
    active_t = lax.optimization_barrier(active.T)
    act_sum = jnp.sum(active.astype(jnp.float32), axis=0)

    grad_dec_bias = jnp.concatenate(
        [
            factor * jnp.sum(all_residual[:, l * width : (l + 1) * width].astype(jnp.float32), axis=0, keepdims=True)
            for l in range(layers)
        ],
        axis=0,
    )
    backward = jnp.dot(all_residual, dec_t, preferred_element_type=jnp.float32)
    grad_act = factor * backward + sparsity_weight / total_rows * dec_norm
    grad_before = jnp.where(before > 0.0, grad_act, 0.0).astype(jnp.bfloat16)
    grad_enc = jnp.dot(gathered_t, grad_before, preferred_element_type=jnp.float32).astype(jnp.bfloat16)
    grad_enc_bias = jnp.sum(grad_before.astype(jnp.float32), axis=0)
    pieces = []
    for l in range(layers):
        total = jnp.dot(
            active_t, all_residual[:, l * width : (l + 1) * width], preferred_element_type=jnp.float32
        )
        scale = sparsity_weight / total_rows * act_sum * inv_norm[l]
        pieces.append((factor * total + scale[:, None] * layer_dec[l]).astype(jnp.bfloat16))
    pieces = lax.optimization_barrier(pieces)
    grad_dec = jnp.stack(pieces, axis=1)
    return (
        own_residual.reshape(tok_dev, layers, width),
        grad_enc.reshape(layers, width, lat_dev),
        grad_enc_bias,
        grad_dec,
        grad_dec_bias,
    )


def solution(mesh):
    return jax.shard_map(
        body,
        mesh=mesh,
        in_specs=(
            P(("grp", "lat"), None, None),
            P("grp", None, "lat"),
            P(("grp", "lat")),
            P("lat", "grp", None),
            P("grp", None),
        ),
        out_specs=(
            P(("grp", "lat"), None, None),
            P("grp", None, "lat"),
            P(("grp", "lat")),
            P("lat", "grp", None),
            P("grp", None),
        ),
        check_vma=False,
    )
```
